256 devices in a mesh: energy: 32 (over x, z_hi, core), space: 8 (over y, z_lo).
Axes of the slice: x: 4, y: 4, z: 8 (z_hi: 4, z_lo: 2; z = z_hi * 2 + z_lo), core: 2. Of those that a mesh axis runs over, the one named last changes fastest.
Arguments:
- g_lesser: float32 [2, 256, 8, 256, 256], P(None, 'energy', 'space'), may hold values from -6 to 6
- g_greater: float32 [2, 256, 8, 256, 256], P(None, 'energy', 'space'), may hold values from -6 to 6
- v_diag: float32 [8, 256, 256], P('space'), may hold values from -0.375 to 0.375
- v_upper: float32 [8, 256, 256], P('space'), may hold values from -0.375 to 0.375
Outputs:
- screened: float32 [2, 64, 8, 256, 256], P(None, 'energy', 'space')
The draws below stay inside these ranges and needn't reach their ends.
All inputs are finite; a program needn't handle non-finite values.
Results may differ from the reference program's by a relative error of at most 0.000098.
Values sent between devices are 32-bit elements; how exact they have to be, the bound alone decides.
No kernel may reach another device: no remote copies, remote signals or barrier semaphores. Data moves between devices by JAX's collectives and lax.ppermute only.
A program may use at most 128 MiB of HBM per device.

```python
import math
import jax
import jax.numpy as jnp
from jax import lax

NE = 256
NW = 64
B = 256
NB = 8


def steps_of(rng, shape, shards, smallest, top_value):
    level, own = 1.0, jax.random.fold_in(rng, 6)
    for dim, parts in shards:
        heights = jnp.exp(jax.random.uniform(jax.random.fold_in(own, dim), (parts,), jnp.float32, smallest / len(shards), top_value / len(shards)))
        level = level * jnp.repeat(heights, shape[dim] // parts).reshape([-1 if axis == dim else 1 for axis in range(len(shape))])
    return level


def scatter_about(rng, extent, width, limit, shards=(), kind=jnp.bfloat16):
    drawn = width * jax.random.normal(rng, extent, jnp.float32)
    if shards:
        drawn = drawn * steps_of(rng, extent, shards, -0.22, 0.18)
    return jnp.clip(drawn, -limit, limit).astype(kind)


def setup_inputs(seed: int = 0) -> dict:
    key_of = jax.random.split(jax.random.key(seed), 5)
    return {
        "g_lesser": scatter_about(key_of[0], (2, NE, NB, B, B), 1.0, 6.0, ((1, 32), (2, 8)), jnp.float32),
        "g_greater": scatter_about(key_of[1], (2, NE, NB, B, B), 1.0, 6.0, ((1, 32), (2, 8)), jnp.float32),
        "v_diag": scatter_about(key_of[2], (NB, B, B), B ** -0.5, 0.375, ((0, 8),), jnp.float32),
        "v_upper": scatter_about(key_of[3], (NB, B, B), B ** -0.5, 0.375, ((0, 8),), jnp.float32),
    }


prefactor = 0.0625


def tables(count):
    length = 2 * count
    freqs = jnp.arange(length, dtype=jnp.int32)[:, None]
    points = jnp.arange(count, dtype=jnp.int32)[None, :]
    phase = (2.0 * math.pi / length) * ((freqs * points) % length).astype(jnp.float32)
    return jnp.cos(phase), jnp.sin(phase)


def product(left, right):
    return jnp.dot(left, right, precision=lax.Precision.HIGHEST, preferred_element_type=jnp.float32)


def correlate(lesser, greater, keep):
    count = lesser.shape[1]
    rest = tuple(lesser.shape[2:])
    lesser = lesser.reshape(2, count, -1)
    greater = greater.reshape(2, count, -1)
    cosine, sine = tables(count)
    less_re = product(cosine, lesser[0]) + product(sine, lesser[1])
    less_im = product(cosine, lesser[1]) - product(sine, lesser[0])
    great_re = product(cosine, greater[0]) - product(sine, greater[1])
    great_im = product(cosine, greater[1]) + product(sine, greater[0])
    spec_re = less_re * great_re - less_im * great_im
    spec_im = less_re * great_im + less_im * great_re
    factor = prefactor / (2 * count)
    back_cos = cosine.T[:keep]
    back_sin = sine.T[:keep]
    out_re = (product(back_cos, spec_re) - product(back_sin, spec_im)) * factor
    out_im = (product(back_cos, spec_im) + product(back_sin, spec_re)) * factor
    return jnp.stack([out_re, out_im]).reshape((2, keep) + rest)


def sandwich(left, middle, right):
    halfway = jnp.einsum('rab,...rbd->...rad', left, middle, precision=lax.Precision.HIGHEST)
    return jnp.einsum('...rad,rdf->...raf', halfway, right, precision=lax.Precision.HIGHEST)


def reference(g_lesser, g_greater, v_diag, v_upper):
    flipped = jnp.swapaxes(g_greater, 3, 4)

    def one_row(pair):
        return correlate(pair[0], pair[1], NW)

    rows = lax.map(one_row, (jnp.moveaxis(g_lesser, 2, 0), jnp.moveaxis(flipped, 2, 0)))
    polar = jnp.moveaxis(rows, 0, 2)
    uppers_before = jnp.concatenate([jnp.zeros((1,) + tuple(v_upper.shape[1:]), jnp.float32), v_upper[:-1]], axis=0)
    upper_swapped = jnp.swapaxes(v_upper, 1, 2)
    before_swapped = jnp.swapaxes(uppers_before, 1, 2)

    def one_energy(block):
        padded = jnp.pad(block, ((0, 0), (1, 1), (0, 0), (0, 0)))
        own_term = sandwich(v_diag, block, v_diag)
        above_term = sandwich(before_swapped, padded[:, :-2], uppers_before)
        below_term = sandwich(v_upper, padded[:, 2:], upper_swapped)
        return own_term + above_term + below_term

    result = lax.map(one_energy, jnp.moveaxis(polar, 1, 0))
    return jnp.moveaxis(result, 0, 1)
```

```python
import numpy as np

import jax
import jax.numpy as jnp
from jax import lax
from jax.experimental import pallas as pl
from jax.experimental.layout import Layout, with_layout_constraint
from jax.experimental.pallas import tpu as pltpu
from jax.sharding import Mesh
from jax.sharding import PartitionSpec as P

NW = 64
PREFACTOR = 0.0625
CORES, PAIR = 2, 2
ENERGY = ("xz", "core")
SPACE = ("y", "zl")


def halves(table):
    high = table.astype(jnp.bfloat16)
    low = (table - high.astype(np.float64)).astype(jnp.bfloat16)
    return np.concatenate([high, high, low], axis=1)


def tables(block):
    length = 2 * block
    freqs = np.concatenate([np.arange(0, length, 2), np.arange(1, length, 2)])
    phase = 2.0 * np.pi / length * (np.outer(freqs, np.arange(block)) % length)
    c, s = np.cos(phase), np.sin(phase)
    lesser = np.block([[c, s], [-s, c]])
    greater = np.block([[c, -s], [s, c]])
    back = np.block([[c.T, -s.T], [s.T, c.T]]) * (PREFACTOR / length)
    return halves(lesser), halves(greater), halves(back)


def split(x):
    high = x.astype(jnp.bfloat16)
    low = (x - high.astype(jnp.float32)).astype(jnp.bfloat16)
    return high, low


def dot(left, right):
    return jnp.dot(left, right, preferred_element_type=jnp.float32)


def correlate_row(less_re, less_im, great_re, great_im, t_less, t_great, t_back):
    block = NW
    count = less_re.shape[0] // block
    parts = [split(x) for x in (less_re, less_im, great_re, great_im)]

    def spectrum(table, re, im, j):
        rows = slice(j * block, (j + 1) * block)
        high = [re[0][rows], im[0][rows]]
        low = [re[1][rows], im[1][rows]]
        return dot(table, jnp.concatenate(high + low + high, axis=0))

    acc_re = acc_im = None
    before = None
    for j in range(count):
        less = spectrum(t_less, parts[0], parts[1], j)
        great = spectrum(t_great, parts[2], parts[3], j)
        if before is None:
            w_re, w_im = great[: 2 * block], great[2 * block :]
        else:
            w_re = jnp.concatenate(
                [great[:block] + before[:block], great[block : 2 * block] - before[block : 2 * block]], axis=0
            )
            w_im = jnp.concatenate(
                [
                    great[2 * block : 3 * block] + before[2 * block : 3 * block],
                    great[3 * block :] - before[3 * block :],
                ],
                axis=0,
            )
        l_re, l_im = less[: 2 * block], less[2 * block :]
        re = l_re * w_re - l_im * w_im
        im = l_re * w_im + l_im * w_re
        acc_re = re if acc_re is None else acc_re + re
        acc_im = im if acc_im is None else acc_im + im
        before = great
    high, low = split(jnp.concatenate([acc_re, acc_im], axis=0))
    return dot(t_back, jnp.concatenate([high, low, high], axis=0))


def kernel(less_ref, great_ref, t_less, t_great, t_back, out_ref):
    energies = less_ref.shape[0] * less_ref.shape[3]
    columns = less_ref.shape[4]
    less = [less_ref[:, 0, c].reshape(energies, columns) for c in range(2)]
    great = [great_ref[:, 0, c].reshape(energies, columns) for c in range(2)]
    out = correlate_row(*less, *great, t_less[...], t_great[...], t_back[...])
    out_ref[0] = out.reshape(2, NW, columns)


def correlate(less, great):
    sources, rows, _, local, columns = less.shape
    consts = [jnp.asarray(t) for t in tables(NW)]
    spec = pl.BlockSpec((sources, 1, 2, local, columns), lambda i: (0, i, 0, 0, 0))
    fixed = [pl.BlockSpec(t.shape, lambda i: (0, 0)) for t in consts]
    return pl.pallas_call(
        kernel,
        grid=(rows,),
        in_specs=[spec, spec] + fixed,
        out_specs=pl.BlockSpec((1, 2, NW, columns), lambda i: (i, 0, 0, 0)),
        out_shape=jax.ShapeDtypeStruct((rows, 2, NW, columns), jnp.float32),
        compiler_params=pltpu.CompilerParams(
            dimension_semantics=("arbitrary",), vmem_limit_bytes=40 * 1024 * 1024
        ),
        cost_estimate=pl.CostEstimate(
            flops=4_000_000_000, bytes_accessed=9_500_000, transcendentals=0
        ),
    )(less, great, *consts)


def tripled(x, axis, order):
    parts = split(x)
    return jnp.concatenate([parts[i] for i in order], axis=axis)


def sandwich(left, middle, right):
    left = tripled(left, 1, (0, 0, 1))
    right = tripled(right, 0, (0, 1, 0))
    halfway = [dot(left, tripled(m, 0, (0, 1, 0))) for m in middle]
    return [dot(tripled(h, 1, (0, 0, 1)), right) for h in halfway]


def block_of(ref, *index):
    return ref[index].reshape(-1, ref.shape[-1])


def pair_kernel(even_ref, polar_ref, v0, v1, u0, u0_t, own_ref, send_ref):
    p0 = [block_of(polar_ref, slice(None), 0, c) for c in range(2)]
    p1 = [block_of(polar_ref, slice(None), 1, c) for c in range(2)]
    even = even_ref[0] == 1
    s0 = [x + y for x, y in zip(sandwich(v0[...], p0, v0[...]), sandwich(u0[...], p1, u0_t[...]))]
    s1 = [x + y for x, y in zip(sandwich(v1[...], p1, v1[...]), sandwich(u0_t[...], p0, u0[...]))]
    for c in range(2):
        own_ref[c] = jnp.where(even, s0[c], s1[c])
        send_ref[c] = jnp.where(even, s1[c], s0[c])


def outer_kernel(pick_ref, part_ref, before_ref, after_ref, left, right, out_ref):
    after = pick_ref[0] == 1
    p = [
        jnp.where(after, block_of(after_ref, slice(None), c), block_of(before_ref, slice(None), c))
        for c in range(2)
    ]
    term = sandwich(left[...], p, right[...])
    for c in range(2):
        out_ref[c] = part_ref[c] + term[c]


def on_core(body, outs, flops, scalars, *arrays):
    vmem = pl.BlockSpec(memory_space=pltpu.VMEM)
    smem = pl.BlockSpec(memory_space=pltpu.SMEM)
    size = sum(4 * x.size for x in arrays)
    return pl.pallas_call(
        body,
        in_specs=[smem] * len(scalars) + [vmem] * len(arrays),
        out_specs=[vmem] * len(outs),
        out_shape=outs,
        compiler_params=pltpu.CompilerParams(vmem_limit_bytes=40 * 1024 * 1024),
        cost_estimate=pl.CostEstimate(flops=flops, bytes_accessed=size, transcendentals=0),
    )(*scalars, *arrays)


SWAP = [(0, 1), (1, 0)]


def plain(x):
    return with_layout_constraint(x, Layout(major_to_minor=tuple(range(x.ndim))))


def local(g_lesser, g_greater, v_diag, v_upper):
    devices = lax.axis_size(ENERGY)
    size = g_lesser.shape[3]
    rows = size // devices
    length = lax.axis_size("y")
    forward = [(i, i + 1) for i in range(length - 1)]
    backward = [(j, i) for i, j in forward]

    def exchange(block):
        got = lax.all_to_all(block, ENERGY, split_axis=0, concat_axis=0, tiled=True)
        return got.reshape((devices, rows) + block.shape[1:])

    first_core = lax.axis_index("core") == 0
    even = lax.axis_index("zl") == 0
    v, u = v_diag[0], v_upper[0]
    theirs = lax.ppermute(jnp.where(first_core, v, u), "zl", SWAP)
    less_send, theirs = lax.optimization_barrier((g_lesser[:, :, 0].transpose(2, 0, 1, 3), theirs))
    less = exchange(less_send)

    other = lax.ppermute(theirs, "core", SWAP)
    v_pair = jnp.where(first_core, theirs, other)
    u_pair = jnp.where(first_core, other, theirs)
    v0, v1 = jnp.where(even, v, v_pair), jnp.where(even, v_pair, v)
    u0, u1 = jnp.where(even, u, u_pair), jnp.where(even, u_pair, u)
    u_before_t = lax.ppermute(u1, "y", forward).T
    own_left, send_left = jnp.where(even, u_before_t, u1), jnp.where(even, u1, u_before_t)

    great_send = g_greater[:, :, 0].transpose(3, 0, 1, 2)
    great_send, v0, v1, u0, u0_t, own_left, own_right, send_left, send_right = lax.optimization_barrier(
        (great_send, v0, v1, u0, u0.T, own_left, own_left.T, send_left, send_left.T)
    )
    great = exchange(great_send)

    polar = correlate(less, great)
    polar = lax.all_to_all(
        plain(polar.transpose(2, 1, 0, 3)), ENERGY + ("zl",), split_axis=0, concat_axis=0, tiled=True
    )
    polar = polar.reshape(devices, PAIR, 2, rows, size)
    p_before = lax.ppermute(polar[:, 1], "y", forward)
    p_after = lax.ppermute(polar[:, 0], "y", backward)

    flag = even.astype(jnp.int32).reshape(1)
    result = jax.ShapeDtypeStruct((2, size, size), jnp.float32)
    own, send = on_core(
        pair_kernel, [result, result], 3_200_000_000, [flag], polar, v0, v1, u0, u0_t
    )
    outer = (p_before, p_after)
    (send,) = on_core(
        outer_kernel, [result], 800_000_000, [flag], send, *outer, send_left, send_right
    )
    got = lax.ppermute(send, "zl", SWAP)
    (own,) = on_core(
        outer_kernel, [result], 800_000_000, [1 - flag], own, *outer, own_left, own_right
    )
    return jnp.stack([jnp.where(even, own, got), jnp.where(even, got, own)], axis=1)[:, :, None]


def solution(mesh):
    count, width = mesh.devices.shape
    fine = Mesh(
        mesh.devices.reshape(count // CORES, CORES, width // PAIR, PAIR), ENERGY + SPACE
    )
    blocks = P(None, ENERGY, SPACE, None, None)
    rows = P(SPACE, None, None)
    return jax.shard_map(
        local, mesh=fine, in_specs=(blocks, blocks, rows, rows), out_specs=blocks, check_vma=False
    )
```

```python
import functools

import numpy as np

import jax
import jax.numpy as jnp
from jax import lax
from jax.experimental import pallas as pl
from jax.experimental.layout import Layout, with_layout_constraint
from jax.experimental.pallas import tpu as pltpu
from jax.sharding import Mesh
from jax.sharding import PartitionSpec as P

NW = 64
LANES = 128
PREFACTOR = 0.0625
CORES, PAIR = 2, 2
ENERGY = ("xz", "core")
SPACE = ("y", "zl")


def cut(table):
    high = table.astype(jnp.bfloat16)
    return high, (table - high.astype(np.float64)).astype(jnp.bfloat16)


def tables(block):
    length = 2 * block
    freqs = np.concatenate([np.arange(0, block, 2), np.arange(1, block, 2)])
    odd = 2 * freqs + 1
    phase = np.pi / length * (np.outer(odd, np.arange(block)) % (2 * length))
    c, s = np.cos(phase), np.sin(phase)
    high, low = cut(np.concatenate([c, s], axis=0))
    there = np.concatenate([high, high, low, low], axis=1)
    high, low = cut(np.concatenate([c.T, s.T], axis=1) * (PREFACTOR / length))
    return there, np.concatenate([high, high, low], axis=1)


def split(x):
    high = x.astype(jnp.bfloat16)
    low = (x - high.astype(jnp.float32)).astype(jnp.bfloat16)
    return high, low


def dot(left, right):
    return jnp.dot(left, right, preferred_element_type=jnp.float32)


def spectrum(there, re, im, sign):
    both = split(jnp.concatenate([re, im], axis=1))
    sums = dot(there, jnp.concatenate([both[0], both[1], both[0], both[1]], axis=0))
    half, columns = sums.shape[0] // 2, re.shape[1]
    c_re, c_im = sums[:half, :columns], sums[:half, columns:]
    s_re, s_im = sums[half:, :columns], sums[half:, columns:]
    minus = (c_re - s_im, c_im + s_re)
    plus = (c_re + s_im, c_im - s_re)
    first, second = (plus, minus) if sign < 0 else (minus, plus)
    return tuple(jnp.concatenate([p, q], axis=0) for p, q in zip(first, second))


def shifted(now, before):
    n_re, n_im = now
    b_re, b_im = before
    quarter = n_re.shape[0] // 4
    re, im = [], []
    for part, sign in enumerate((1, -1, -1, 1)):
        rows = slice(part * quarter, (part + 1) * quarter)
        if sign > 0:
            re.append(n_re[rows] + b_im[rows])
            im.append(n_im[rows] - b_re[rows])
        else:
            re.append(n_re[rows] - b_im[rows])
            im.append(n_im[rows] + b_re[rows])
    return jnp.concatenate(re, axis=0), jnp.concatenate(im, axis=0)


def polar_row(less_re, less_im, great_re, great_im, there, back):
    re = im = before = None
    for j in range(great_re.shape[0] // NW):
        rows = slice(j * NW, (j + 1) * NW)
        great = spectrum(there, great_re[rows], great_im[rows], 1)
        w_re, w_im = great if before is None else shifted(great, before)
        l_re, l_im = spectrum(there, less_re[rows], less_im[rows], -1)
        p_re = l_re * w_re - l_im * w_im
        p_im = l_re * w_im + l_im * w_re
        re, im = (p_re, p_im) if re is None else (re + p_re, im + p_im)
        before = great
    half = NW
    real = jnp.concatenate([re[:half] + re[half:], im[half:] - im[:half]], axis=0)
    imag = jnp.concatenate([im[:half] + im[half:], re[:half] - re[half:]], axis=0)
    high, low = split(jnp.concatenate([real, imag], axis=1))
    out = dot(back, jnp.concatenate([high, low, high], axis=0))
    return out[:, : re.shape[1]], out[:, re.shape[1] :]


def polar_kernel(less_hbm, great_hbm, there, back, out_ref, held, sems):
    rows = held.shape[1]

    def copy(which, i):
        source = (less_hbm, great_hbm)[which]
        return pltpu.make_async_copy(source.at[:, i], held.at[which, i], sems.at[which, i])

    for i in range(rows):
        copy(0, i).start()
        copy(1, i).start()

    def row(i, carry):
        copy(0, i).wait()
        copy(1, i).wait()
        parts = [held[k, i, :, c].reshape(-1, held.shape[-1]) for k in range(2) for c in range(2)]
        for c, part in enumerate(polar_row(*parts, there[...], back[...])):
            wide = part.shape[1] // LANES
            for h in range(wide):
                place = pl.ds((c * wide + h) * rows + i, NW, stride=2 * wide * rows)
                out_ref[place, :] = part[:, h * LANES : (h + 1) * LANES]
        return carry

    lax.fori_loop(0, rows, row, 0)


def polar_of(less, great):
    sources, rows, _, local, columns = great.shape
    there, back = (jnp.asarray(t) for t in tables(NW))
    hbm = pl.BlockSpec(memory_space=pltpu.HBM)
    vmem = pl.BlockSpec(memory_space=pltpu.VMEM)
    out = pl.pallas_call(
        polar_kernel,
        in_specs=[hbm, hbm, vmem, vmem],
        out_specs=vmem,
        out_shape=jax.ShapeDtypeStruct((NW * 2 * rows * columns // LANES, LANES), jnp.float32),
        scratch_shapes=[
            pltpu.VMEM((2, rows, sources, 2, local, columns), jnp.float32),
            pltpu.SemaphoreType.DMA((2, rows)),
        ],
        compiler_params=pltpu.CompilerParams(vmem_limit_bytes=57 * 1024 * 1024),
        cost_estimate=pl.CostEstimate(
            flops=4_000_000_000, bytes_accessed=9_500_000, transcendentals=0
        ),
    )(less, great, there, back)
    return out.reshape(NW, 2, columns // LANES, rows, LANES)


def tripled(x, axis, order):
    parts = split(x)
    return jnp.concatenate([parts[i] for i in order], axis=axis)


def sandwich(left, middle, right):
    left = tripled(left, 1, (0, 0, 1))
    right = tripled(right, 0, (0, 1, 0))
    halfway = [dot(left, tripled(m, 0, (0, 1, 0))) for m in middle]
    return [dot(tripled(h, 1, (0, 0, 1)), right) for h in halfway]


def block_of(ref, *index):
    wide = ref.shape[-3]
    return jnp.concatenate([ref[(slice(None), *index, h)].reshape(-1, LANES) for h in range(wide)], axis=1)


def screen(near, far, outer, v, w, w_t, a, a_t):
    terms = (sandwich(v, near, v), sandwich(w, far, w_t), sandwich(a, outer, a_t))
    return [x + y + z for x, y, z in zip(*terms)]


def send_kernel(c, near, far, outer, v, w, w_t, a, a_t, out_ref):
    blocks = ([block_of(near, c)], [block_of(far, c)], [block_of(outer)])
    (out_ref[...],) = screen(*blocks, v[...], w[...], w_t[...], a[...], a_t[...])


def own_kernel(near, far, outer, v, w, w_t, a, a_t, out_ref):
    blocks = [[block_of(ref, c) for c in range(2)] for ref in (near, far, outer)]
    out_ref[0], out_ref[1] = screen(*blocks, v[...], w[...], w_t[...], a[...], a_t[...])


def on_core(body, shape, flops, *arrays):
    vmem = pl.BlockSpec(memory_space=pltpu.VMEM)
    return pl.pallas_call(
        body,
        in_specs=[vmem] * len(arrays),
        out_specs=vmem,
        out_shape=jax.ShapeDtypeStruct(shape, jnp.float32),
        compiler_params=pltpu.CompilerParams(vmem_limit_bytes=16 * 1024 * 1024),
        cost_estimate=pl.CostEstimate(
            flops=flops, bytes_accessed=sum(4 * x.size for x in arrays), transcendentals=0
        ),
    )(*arrays)


SWAP = [(0, 1), (1, 0)]


def plain(x):
    return with_layout_constraint(x, Layout(major_to_minor=tuple(range(x.ndim))))


def local(g_lesser, g_greater, v_diag, v_upper):
    devices = lax.axis_size(ENERGY)
    size = g_lesser.shape[3]
    rows = size // devices
    length = lax.axis_size("y")
    forward = [(i, i + 1) for i in range(length - 1)]

    first_core = lax.axis_index("core") == 0
    even = lax.axis_index("zl") == 0
    v, u = v_diag[0], v_upper[0]
    theirs = lax.ppermute(plain(jnp.where(first_core, v, u)), "zl", SWAP)
    less_send = g_lesser.reshape(2, -1, devices, rows, size).transpose(2, 0, 1, 3, 4)
    less_send, theirs = lax.optimization_barrier((plain(less_send), theirs))
    less = plain(lax.all_to_all(plain(less_send), ENERGY, split_axis=0, concat_axis=0, tiled=True))

    other = lax.ppermute(theirs, "core", SWAP)
    v_pair = jnp.where(first_core, theirs, other)
    u_pair = jnp.where(first_core, other, theirs)
    u0, u1 = jnp.where(even, u, u_pair), jnp.where(even, u_pair, u)
    before_t = plain(lax.ppermute(plain(u1), "y", forward)).T
    u0_t = u0.T
    w, w_t = jnp.where(even, u0_t, u0), jnp.where(even, u0, u0_t)
    sends, keeps = jnp.where(even, u1, before_t), jnp.where(even, before_t, u1)
    fixed = tuple(plain(x) for x in (v, v_pair, w, w_t, sends, sends.T, keeps, keeps.T))

    great_send = g_greater[:, :, 0].transpose(3, 0, 1, 2)
    great_send, fixed = lax.optimization_barrier((great_send, fixed))
    v_own, v_pair, w, w_t, sends, sends_t, keeps, keeps_t = fixed
    great = lax.all_to_all(great_send, ENERGY, split_axis=0, concat_axis=0, tiled=True)
    great = great.reshape((devices, rows) + great.shape[1:])

    polar = polar_of(plain(less.transpose(0, 3, 1, 2, 4)), great)
    polar = lax.all_to_all(
        plain(polar), ENERGY + ("zl",), split_axis=0, concat_axis=0, tiled=True
    )
    polar = polar.reshape((devices, PAIR) + polar.shape[1:])

    pair = [(i, l) for i in range(length) for l in range(PAIR)]
    number = {p: n for n, p in enumerate(pair)}
    toward, away = [], []
    for i, l in pair:
        step = 1 - 2 * l
        for route, target in ((toward, (i - step, l)), (away, (i + step, l))):
            if target in number:
                route.append((number[i, l], number[target]))
    near = plain(jnp.where(even, polar[:, 1], polar[:, 0]))
    far = plain(jnp.where(even, polar[:, 0], polar[:, 1]))
    for_send = [lax.ppermute(plain(far[:, c]), SPACE, toward) for c in range(2)]

    got = []
    for c in range(2):
        ready = on_core(
            functools.partial(send_kernel, c), (size, size), 600_000_000,
            near, far, for_send[c], v_pair, w, w_t, sends, sends_t,
        )
        if c == 0:
            ready, near_later = lax.optimization_barrier((ready, near))
            for_own = lax.ppermute(near_later, SPACE, away)
        got.append(plain(lax.ppermute(plain(ready), "zl", SWAP)))
    kept = on_core(
        own_kernel, (2, size, size), 1_200_000_000, far, near, for_own, v_own, w_t, w, keeps, keeps_t
    )
    out = []
    for c in range(2):
        out += [jnp.where(even, kept[c], got[c]), jnp.where(even, got[c], kept[c])]
    return plain(jnp.stack(out).reshape(2, PAIR, 1, size, size))


def solution(mesh):
    count, width = mesh.devices.shape
    fine = Mesh(
        mesh.devices.reshape(count // CORES, CORES, width // PAIR, PAIR), ENERGY + SPACE
    )
    blocks = P(None, ENERGY, SPACE, None, None)
    rows = P(SPACE, None, None)
    return jax.shard_map(
        local, mesh=fine, in_specs=(blocks, blocks, rows, rows), out_specs=blocks, check_vma=False
    )
```

```python
import functools

import numpy as np

import jax
import jax.numpy as jnp
from jax import lax
from jax.experimental import pallas as pl
from jax.experimental.layout import Layout, with_layout_constraint
from jax.experimental.pallas import tpu as pltpu
from jax.sharding import Mesh
from jax.sharding import PartitionSpec as P


NW = 64
LANES = 128
PREFACTOR = 0.0625
CORES, PAIR = 2, 2
ENERGY = ("xz", "core")
SPACE = ("y", "zl")


def cut(table):
    high = table.astype(jnp.bfloat16)
    return high, (table - high.astype(np.float64)).astype(jnp.bfloat16)


def tables(block):
    length = 2 * block
    freqs = np.concatenate([np.arange(0, block, 2), np.arange(1, block, 2)])
    odd = 2 * freqs + 1
    phase = np.pi / length * (np.outer(odd, np.arange(block)) % (2 * length))
    c, s = np.cos(phase), np.sin(phase)
    high, low = cut(np.concatenate([c, s], axis=0))
    there = np.concatenate([high, high, low, low], axis=1)
    high, low = cut(np.concatenate([c.T, s.T], axis=1) * (PREFACTOR / length))
    return there, np.concatenate([high, high, low], axis=1)


def split(x):
    high = x.astype(jnp.bfloat16)
    low = (x - high.astype(jnp.float32)).astype(jnp.bfloat16)
    return high, low


def dot(left, right):
    return jnp.dot(left, right, preferred_element_type=jnp.float32)


def spectrum(there, re, im, sign):
    both = split(jnp.concatenate([re, im], axis=1))
    sums = dot(there, jnp.concatenate([both[0], both[1], both[0], both[1]], axis=0))
    half, columns = sums.shape[0] // 2, re.shape[1]
    c_re, c_im = sums[:half, :columns], sums[:half, columns:]
    s_re, s_im = sums[half:, :columns], sums[half:, columns:]
    minus = (c_re - s_im, c_im + s_re)
    plus = (c_re + s_im, c_im - s_re)
    first, second = (plus, minus) if sign < 0 else (minus, plus)
    return tuple(jnp.concatenate([p, q], axis=0) for p, q in zip(first, second))


def shifted(now, before):
    n_re, n_im = now
    b_re, b_im = before
    quarter = n_re.shape[0] // 4
    re, im = [], []
    for part, sign in enumerate((1, -1, -1, 1)):
        rows = slice(part * quarter, (part + 1) * quarter)
        if sign > 0:
            re.append(n_re[rows] + b_im[rows])
            im.append(n_im[rows] - b_re[rows])
        else:
            re.append(n_re[rows] - b_im[rows])
            im.append(n_im[rows] + b_re[rows])
    return jnp.concatenate(re, axis=0), jnp.concatenate(im, axis=0)


def polar_row(less_re, less_im, great_re, great_im, there, back):
    re = im = before = None
    for j in range(great_re.shape[0] // NW):
        rows = slice(j * NW, (j + 1) * NW)
        great = spectrum(there, great_re[rows], great_im[rows], 1)
        w_re, w_im = great if before is None else shifted(great, before)
        l_re, l_im = spectrum(there, less_re[rows], less_im[rows], -1)
        p_re = l_re * w_re - l_im * w_im
        p_im = l_re * w_im + l_im * w_re
        re, im = (p_re, p_im) if re is None else (re + p_re, im + p_im)
        before = great
    half = NW
    real = jnp.concatenate([re[:half] + re[half:], im[half:] - im[:half]], axis=0)
    imag = jnp.concatenate([im[:half] + im[half:], re[:half] - re[half:]], axis=0)
    high, low = split(jnp.concatenate([real, imag], axis=1))
    out = dot(back, jnp.concatenate([high, low, high], axis=0))
    return out[:, : re.shape[1]], out[:, re.shape[1] :]


def polar_kernel(less_hbm, great_hbm, there, back, out_ref, held, sems):
    rows = held.shape[1]

    def copy(which, i):
        source = (less_hbm, great_hbm)[which]
        return pltpu.make_async_copy(source.at[:, i], held.at[which, i], sems.at[which, i])

    for i in range(rows):
        copy(0, i).start()
        copy(1, i).start()

    def row(i, carry):
        copy(0, i).wait()
        copy(1, i).wait()
        parts = [held[k, i, :, c].reshape(-1, held.shape[-1]) for k in range(2) for c in range(2)]
        for c, part in enumerate(polar_row(*parts, there[...], back[...])):
            wide = part.shape[1] // LANES
            for h in range(wide):
                place = pl.ds((c * wide + h) * rows + i, NW, stride=2 * wide * rows)
                out_ref[place, :] = part[:, h * LANES : (h + 1) * LANES]
        return carry

    lax.fori_loop(0, rows, row, 0)


def polar_of(less, great):
    sources, rows, _, local, columns = great.shape
    there, back = (jnp.asarray(t) for t in tables(NW))
    hbm = pl.BlockSpec(memory_space=pltpu.HBM)
    vmem = pl.BlockSpec(memory_space=pltpu.VMEM)
    out = pl.pallas_call(
        polar_kernel,
        in_specs=[hbm, hbm, vmem, vmem],
        out_specs=vmem,
        out_shape=jax.ShapeDtypeStruct((NW * 2 * rows * columns // LANES, LANES), jnp.float32),
        scratch_shapes=[
            pltpu.VMEM((2, rows, sources, 2, local, columns), jnp.float32),
            pltpu.SemaphoreType.DMA((2, rows)),
        ],
        compiler_params=pltpu.CompilerParams(vmem_limit_bytes=57 * 1024 * 1024),
        cost_estimate=pl.CostEstimate(
            flops=4_000_000_000, bytes_accessed=9_500_000, transcendentals=0
        ),
    )(less, great, there, back)
    return out.reshape(NW, 2, columns // LANES, rows, LANES)


def tripled(x, axis, order):
    parts = split(x)
    return jnp.concatenate([parts[i] for i in order], axis=axis)


def sandwich(left, middle, right):
    left = tripled(left, 1, (0, 0, 1))
    right = tripled(right, 0, (0, 1, 0))
    halfway = [dot(left, tripled(m, 0, (0, 1, 0))) for m in middle]
    return [dot(tripled(h, 1, (0, 0, 1)), right) for h in halfway]


def block_of(ref, *index):
    wide = ref.shape[-3]
    return jnp.concatenate([ref[(slice(None), *index, h)].reshape(-1, LANES) for h in range(wide)], axis=1)


def screen(near, far, outer, v, w, w_t, a, a_t):
    terms = (sandwich(v, near, v), sandwich(w, far, w_t), sandwich(a, outer, a_t))
    return [x + y + z for x, y, z in zip(*terms)]


def send_kernel(c, near, far, outer, v, w, w_t, a, a_t, out_ref):
    blocks = ([block_of(near, c)], [block_of(far, c)], [block_of(outer)])
    (out_ref[...],) = screen(*blocks, v[...], w[...], w_t[...], a[...], a_t[...])


def own_kernel(near, far, outer, v, w, w_t, a, a_t, out_ref):
    blocks = [[block_of(ref, c) for c in range(2)] for ref in (near, far, outer)]
    out_ref[0], out_ref[1] = screen(*blocks, v[...], w[...], w_t[...], a[...], a_t[...])


def on_core(body, shape, flops, *arrays):
    vmem = pl.BlockSpec(memory_space=pltpu.VMEM)
    return pl.pallas_call(
        body,
        in_specs=[vmem] * len(arrays),
        out_specs=vmem,
        out_shape=jax.ShapeDtypeStruct(shape, jnp.float32),
        compiler_params=pltpu.CompilerParams(vmem_limit_bytes=16 * 1024 * 1024),
        cost_estimate=pl.CostEstimate(
            flops=flops, bytes_accessed=sum(4 * x.size for x in arrays), transcendentals=0
        ),
    )(*arrays)


SWAP = [(0, 1), (1, 0)]


def plain(x):
    return with_layout_constraint(x, Layout(major_to_minor=tuple(range(x.ndim))))


def local(g_lesser, g_greater, v_diag, v_upper):
    devices = lax.axis_size(ENERGY)
    size = g_lesser.shape[3]
    rows = size // devices
    length = lax.axis_size("y")
    forward = [(i, i + 1) for i in range(length - 1)]

    first_core = lax.axis_index("core") == 0
    even = lax.axis_index("zl") == 0
    v, u = v_diag[0], v_upper[0]
    theirs = lax.ppermute(plain(jnp.where(first_core, v, u)), "zl", SWAP)
    less_send = g_lesser.reshape(2, -1, devices, rows, size).transpose(2, 0, 1, 3, 4)
    less_send, theirs = lax.optimization_barrier((plain(less_send), theirs))
    less = plain(lax.all_to_all(plain(less_send), ENERGY, split_axis=0, concat_axis=0, tiled=True))

    other = lax.ppermute(theirs, "core", SWAP)
    v_pair = jnp.where(first_core, theirs, other)
    u_pair = jnp.where(first_core, other, theirs)
    u0, u1 = jnp.where(even, u, u_pair), jnp.where(even, u_pair, u)
    before_t = plain(lax.ppermute(plain(u1), "y", forward)).T
    u0_t = u0.T
    w, w_t = jnp.where(even, u0_t, u0), jnp.where(even, u0, u0_t)
    sends, keeps = jnp.where(even, u1, before_t), jnp.where(even, before_t, u1)
    fixed = tuple(plain(x) for x in (v, v_pair, w, w_t, sends, sends.T, keeps, keeps.T))

    great_send = g_greater[:, :, 0].transpose(3, 0, 1, 2)
    great_send, fixed = lax.optimization_barrier((great_send, fixed))
    v_own, v_pair, w, w_t, sends, sends_t, keeps, keeps_t = fixed
    great = lax.all_to_all(great_send, ENERGY, split_axis=0, concat_axis=0, tiled=True)
    great = great.reshape((devices, rows) + great.shape[1:])

    polar = polar_of(plain(less.transpose(0, 3, 1, 2, 4)), great)
    polar = lax.all_to_all(
        plain(polar), ENERGY + ("zl",), split_axis=0, concat_axis=0, tiled=True
    )
    polar = polar.reshape((devices, PAIR) + polar.shape[1:])

    pair = [(i, l) for i in range(length) for l in range(PAIR)]
    number = {p: n for n, p in enumerate(pair)}
    toward, away = [], []
    for i, l in pair:
        step = 1 - 2 * l
        for route, target in ((toward, (i - step, l)), (away, (i + step, l))):
            if target in number:
                route.append((number[i, l], number[target]))
    near = plain(jnp.where(even, polar[:, 1], polar[:, 0]))
    far = plain(jnp.where(even, polar[:, 0], polar[:, 1]))
    for_send = []
    for c in range(2):
        for_send.append(lax.ppermute(plain(far[:, c]), SPACE, toward))
    for_own = lax.ppermute(near, SPACE, away)

    got = []
    for c in range(2):
        ready = on_core(
            functools.partial(send_kernel, c), (size, size), 600_000_000,
            near, far, for_send[c], v_pair, w, w_t, sends, sends_t,
        )
        got.append(plain(lax.ppermute(plain(ready), "zl", SWAP)))
    kept = on_core(
        own_kernel, (2, size, size), 1_200_000_000, far, near, for_own, v_own, w_t, w, keeps, keeps_t
    )
    out = []
    for c in range(2):
        out += [jnp.where(even, kept[c], got[c]), jnp.where(even, got[c], kept[c])]
    return plain(jnp.stack(out).reshape(2, PAIR, 1, size, size))


def solution(mesh):
    count, width = mesh.devices.shape
    fine = Mesh(
        mesh.devices.reshape(count // CORES, CORES, width // PAIR, PAIR), ENERGY + SPACE
    )
    blocks = P(None, ENERGY, SPACE, None, None)
    rows = P(SPACE, None, None)
    return jax.shard_map(
        local, mesh=fine, in_specs=(blocks, blocks, rows, rows), out_specs=blocks, check_vma=False
    )
```

```python
import functools

import numpy as np

import jax
import jax.numpy as jnp
from jax import lax
from jax.experimental import pallas as pl
from jax.experimental.layout import Layout, with_layout_constraint
from jax.experimental.pallas import tpu as pltpu
from jax.sharding import Mesh
from jax.sharding import PartitionSpec as P


NW = 64
LANES = 128
PREFACTOR = 0.0625
CORES, PAIR = 2, 2
ENERGY = ("xz", "core")
SPACE = ("y", "zl")


def cut(table):
    high = table.astype(jnp.bfloat16)
    return high, (table - high.astype(np.float64)).astype(jnp.bfloat16)


def tables(block):
    length = 2 * block
    freqs = np.concatenate([np.arange(0, block, 2), np.arange(1, block, 2)])
    odd = 2 * freqs + 1
    phase = np.pi / length * (np.outer(odd, np.arange(block)) % (2 * length))
    c, s = np.cos(phase), np.sin(phase)
    high, low = cut(np.concatenate([c, s], axis=0))
    there = np.concatenate([high, high, low, low], axis=1)
    high, low = cut(np.concatenate([c.T, s.T], axis=1) * (PREFACTOR / length))
    return there, np.concatenate([high, high, low], axis=1)


def split(x):
    high = x.astype(jnp.bfloat16)
    low = (x - high.astype(jnp.float32)).astype(jnp.bfloat16)
    return high, low


def dot(left, right):
    return jnp.dot(left, right, preferred_element_type=jnp.float32)


def spectrum(there, re, im, sign):
    both = split(jnp.concatenate([re, im], axis=1))
    sums = dot(there, jnp.concatenate([both[0], both[1], both[0], both[1]], axis=0))
    half, columns = sums.shape[0] // 2, re.shape[1]
    c_re, c_im = sums[:half, :columns], sums[:half, columns:]
    s_re, s_im = sums[half:, :columns], sums[half:, columns:]
    minus = (c_re - s_im, c_im + s_re)
    plus = (c_re + s_im, c_im - s_re)
    first, second = (plus, minus) if sign < 0 else (minus, plus)
    return tuple(jnp.concatenate([p, q], axis=0) for p, q in zip(first, second))


def shifted(now, before):
    n_re, n_im = now
    b_re, b_im = before
    quarter = n_re.shape[0] // 4
    re, im = [], []
    for part, sign in enumerate((1, -1, -1, 1)):
        rows = slice(part * quarter, (part + 1) * quarter)
        if sign > 0:
            re.append(n_re[rows] + b_im[rows])
            im.append(n_im[rows] - b_re[rows])
        else:
            re.append(n_re[rows] - b_im[rows])
            im.append(n_im[rows] + b_re[rows])
    return jnp.concatenate(re, axis=0), jnp.concatenate(im, axis=0)


def polar_row(less_re, less_im, great_re, great_im, there, back):
    re = im = before = None
    for j in range(great_re.shape[0] // NW):
        rows = slice(j * NW, (j + 1) * NW)
        great = spectrum(there, great_re[rows], great_im[rows], 1)
        w_re, w_im = great if before is None else shifted(great, before)
        l_re, l_im = spectrum(there, less_re[rows], less_im[rows], -1)
        p_re = l_re * w_re - l_im * w_im
        p_im = l_re * w_im + l_im * w_re
        re, im = (p_re, p_im) if re is None else (re + p_re, im + p_im)
        before = great
    half = NW
    real = jnp.concatenate([re[:half] + re[half:], im[half:] - im[:half]], axis=0)
    imag = jnp.concatenate([im[:half] + im[half:], re[:half] - re[half:]], axis=0)
    high, low = split(jnp.concatenate([real, imag], axis=1))
    out = dot(back, jnp.concatenate([high, low, high], axis=0))
    return out[:, : re.shape[1]], out[:, re.shape[1] :]


def polar_kernel(less_hbm, great_hbm, there_hbm, back_hbm, out_ref, held, there, back, sems):
    rows = held.shape[1]

    def copy(which, i):
        source = (less_hbm, great_hbm)[which]
        return pltpu.make_async_copy(source.at[:, i], held.at[which, i], sems.at[which, i])

    fixed = (
        pltpu.make_async_copy(there_hbm, there, sems.at[0, rows]),
        pltpu.make_async_copy(back_hbm, back, sems.at[1, rows]),
    )
    for table in fixed:
        table.start()
    for i in range(rows):
        copy(0, i).start()
        copy(1, i).start()
    for table in fixed:
        table.wait()

    def row(i, carry):
        copy(0, i).wait()
        copy(1, i).wait()
        parts = [held[k, i, :, c].reshape(-1, held.shape[-1]) for k in range(2) for c in range(2)]
        for c, part in enumerate(polar_row(*parts, there[...], back[...])):
            wide = part.shape[1] // LANES
            for h in range(wide):
                place = pl.ds((c * wide + h) * rows + i, NW, stride=2 * wide * rows)
                out_ref[place, :] = part[:, h * LANES : (h + 1) * LANES]
        return carry

    lax.fori_loop(0, rows, row, 0)


def polar_of(less, great):
    sources, rows, _, local, columns = great.shape
    there, back = (jnp.asarray(t) for t in tables(NW))
    hbm = pl.BlockSpec(memory_space=pltpu.HBM)
    vmem = pl.BlockSpec(memory_space=pltpu.VMEM)
    out = pl.pallas_call(
        polar_kernel,
        in_specs=[hbm] * 4,
        out_specs=vmem,
        out_shape=jax.ShapeDtypeStruct((NW * 2 * rows * columns // LANES, LANES), jnp.float32),
        scratch_shapes=[
            pltpu.VMEM((2, rows, sources, 2, local, columns), jnp.float32),
            pltpu.VMEM(there.shape, there.dtype),
            pltpu.VMEM(back.shape, back.dtype),
            pltpu.SemaphoreType.DMA((2, rows + 1)),
        ],
        compiler_params=pltpu.CompilerParams(vmem_limit_bytes=57 * 1024 * 1024),
        cost_estimate=pl.CostEstimate(
            flops=4_000_000_000, bytes_accessed=9_500_000, transcendentals=0
        ),
    )(less, great, there, back)
    return out.reshape(NW, 2, columns // LANES, rows, LANES)


def tripled(x, axis, order):
    parts = split(x)
    return jnp.concatenate([parts[i] for i in order], axis=axis)


def sandwich(left, middle, right):
    left = tripled(left, 1, (0, 0, 1))
    right = tripled(right, 0, (0, 1, 0))
    halfway = [dot(left, tripled(m, 0, (0, 1, 0))) for m in middle]
    return [dot(tripled(h, 1, (0, 0, 1)), right) for h in halfway]


def block_of(ref, *index):
    wide = ref.shape[-3]
    return jnp.concatenate([ref[(slice(None), *index, h)].reshape(-1, LANES) for h in range(wide)], axis=1)


def screen(near, far, outer, v, w, w_t, a, a_t):
    terms = (sandwich(v, near, v), sandwich(w, far, w_t), sandwich(a, outer, a_t))
    return [x + y + z for x, y, z in zip(*terms)]


def send_kernel(c, near, far, outer, v, w, w_t, a, a_t, out_ref):
    blocks = ([block_of(near, c)], [block_of(far, c)], [block_of(outer)])
    (out_ref[...],) = screen(*blocks, v[...], w[...], w_t[...], a[...], a_t[...])


def own_kernel(near, far, outer, v, w, w_t, a, a_t, out_ref):
    blocks = [[block_of(ref, c) for c in range(2)] for ref in (near, far, outer)]
    out_ref[0], out_ref[1] = screen(*blocks, v[...], w[...], w_t[...], a[...], a_t[...])


def on_core(body, shape, flops, *arrays):
    vmem = pl.BlockSpec(memory_space=pltpu.VMEM)
    return pl.pallas_call(
        body,
        in_specs=[vmem] * len(arrays),
        out_specs=vmem,
        out_shape=jax.ShapeDtypeStruct(shape, jnp.float32),
        compiler_params=pltpu.CompilerParams(vmem_limit_bytes=16 * 1024 * 1024),
        cost_estimate=pl.CostEstimate(
            flops=flops, bytes_accessed=sum(4 * x.size for x in arrays), transcendentals=0
        ),
    )(*arrays)


SWAP = [(0, 1), (1, 0)]


def plain(x):
    return with_layout_constraint(x, Layout(major_to_minor=tuple(range(x.ndim))))


def local(g_lesser, g_greater, v_diag, v_upper):
    devices = lax.axis_size(ENERGY)
    size = g_lesser.shape[3]
    rows = size // devices
    length = lax.axis_size("y")
    forward = [(i, i + 1) for i in range(length - 1)]

    first_core = lax.axis_index("core") == 0
    even = lax.axis_index("zl") == 0
    v, u = v_diag[0], v_upper[0]
    theirs = lax.ppermute(plain(jnp.where(first_core, v, u)), "zl", SWAP)
    less_send = g_lesser.reshape(2, -1, devices, rows, size).transpose(2, 0, 1, 3, 4)
    less = lax.all_to_all(lax.optimization_barrier(plain(less_send)), ENERGY, split_axis=0, concat_axis=0, tiled=True)
    less = plain(less)

    other = lax.ppermute(theirs, "core", SWAP)
    v_pair = jnp.where(first_core, theirs, other)
    u_pair = jnp.where(first_core, other, theirs)
    u0, u1 = jnp.where(even, u, u_pair), jnp.where(even, u_pair, u)
    before_t = plain(lax.ppermute(plain(u1), "y", forward)).T
    u0_t = u0.T
    w, w_t = jnp.where(even, u0_t, u0), jnp.where(even, u0, u0_t)
    sends, keeps = jnp.where(even, u1, before_t), jnp.where(even, before_t, u1)
    fixed = tuple(plain(x) for x in (v, v_pair, w, w_t, sends, sends.T, keeps, keeps.T))

    great_send = g_greater[:, :, 0].transpose(3, 0, 1, 2)
    great_send, fixed = lax.optimization_barrier((great_send, fixed))
    v_own, v_pair, w, w_t, sends, sends_t, keeps, keeps_t = fixed
    great = lax.all_to_all(great_send, ENERGY, split_axis=0, concat_axis=0, tiled=True)
    great = great.reshape((devices, rows) + great.shape[1:])

    polar = polar_of(plain(less.transpose(0, 3, 1, 2, 4)), great)
    polar = lax.all_to_all(
        plain(polar), ENERGY + ("zl",), split_axis=0, concat_axis=0, tiled=True
    )
    polar = polar.reshape((devices, PAIR) + polar.shape[1:])

    pair = [(i, l) for i in range(length) for l in range(PAIR)]
    number = {p: n for n, p in enumerate(pair)}
    toward, away = [], []
    for i, l in pair:
        step = 1 - 2 * l
        for route, target in ((toward, (i - step, l)), (away, (i + step, l))):
            if target in number:
                route.append((number[i, l], number[target]))
    near = plain(jnp.where(even, polar[:, 1], polar[:, 0]))
    far = plain(jnp.where(even, polar[:, 0], polar[:, 1]))
    for_send = []
    for c in range(2):
        for_send.append(lax.ppermute(plain(far[:, c]), SPACE, toward))
    for_own = lax.ppermute(near, SPACE, away)

    got = []
    for c in range(2):
        ready = on_core(
            functools.partial(send_kernel, c), (size, size), 600_000_000,
            near, far, for_send[c], v_pair, w, w_t, sends, sends_t,
        )
        got.append(plain(lax.ppermute(plain(ready), "zl", SWAP)))
    kept = on_core(
        own_kernel, (2, size, size), 1_200_000_000, far, near, for_own, v_own, w_t, w, keeps, keeps_t
    )
    out = []
    for c in range(2):
        out += [jnp.where(even, kept[c], got[c]), jnp.where(even, got[c], kept[c])]
    return plain(jnp.stack(out).reshape(2, PAIR, 1, size, size))


def solution(mesh):
    count, width = mesh.devices.shape
    fine = Mesh(
        mesh.devices.reshape(count // CORES, CORES, width // PAIR, PAIR), ENERGY + SPACE
    )
    blocks = P(None, ENERGY, SPACE, None, None)
    rows = P(SPACE, None, None)
    return jax.shard_map(
        local, mesh=fine, in_specs=(blocks, blocks, rows, rows), out_specs=blocks, check_vma=False
    )
```

```python
import functools

import numpy as np

import jax
import jax.numpy as jnp
from jax import lax
from jax.experimental import pallas as pl
from jax.experimental.layout import Layout, with_layout_constraint
from jax.experimental.pallas import tpu as pltpu
from jax.sharding import Mesh
from jax.sharding import PartitionSpec as P


NW = 64
LANES = 128
PREFACTOR = 0.0625
CORES, PAIR = 2, 2
ENERGY = ("xz", "core")
SPACE = ("y", "zl")


def cut(table):
    high = table.astype(jnp.bfloat16)
    return high, (table - high.astype(np.float64)).astype(jnp.bfloat16)


def tables(block):
    length = 2 * block
    freqs = np.concatenate([np.arange(0, block, 2), np.arange(1, block, 2)])
    odd = 2 * freqs + 1
    phase = np.pi / length * (np.outer(odd, np.arange(block)) % (2 * length))
    c, s = np.cos(phase), np.sin(phase)
    high, low = cut(np.concatenate([c, s], axis=0))
    there = np.concatenate([high, high, low, low], axis=1)
    high, low = cut(np.concatenate([c.T, s.T], axis=1) * (PREFACTOR / length))
    return there, np.concatenate([high, high, low], axis=1)


def split(x):
    high = x.astype(jnp.bfloat16)
    low = (x - high.astype(jnp.float32)).astype(jnp.bfloat16)
    return high, low


def dot(left, right):
    return jnp.dot(left, right, preferred_element_type=jnp.float32)


def spectrum(there, re, im, sign):
    both = split(jnp.concatenate([re, im], axis=1))
    sums = dot(there, jnp.concatenate([both[0], both[1], both[0], both[1]], axis=0))
    half, columns = sums.shape[0] // 2, re.shape[1]
    c_re, c_im = sums[:half, :columns], sums[:half, columns:]
    s_re, s_im = sums[half:, :columns], sums[half:, columns:]
    minus = (c_re - s_im, c_im + s_re)
    plus = (c_re + s_im, c_im - s_re)
    first, second = (plus, minus) if sign < 0 else (minus, plus)
    return tuple(jnp.concatenate([p, q], axis=0) for p, q in zip(first, second))


def shifted(now, before):
    n_re, n_im = now
    b_re, b_im = before
    quarter = n_re.shape[0] // 4
    re, im = [], []
    for part, sign in enumerate((1, -1, -1, 1)):
        rows = slice(part * quarter, (part + 1) * quarter)
        if sign > 0:
            re.append(n_re[rows] + b_im[rows])
            im.append(n_im[rows] - b_re[rows])
        else:
            re.append(n_re[rows] - b_im[rows])
            im.append(n_im[rows] + b_re[rows])
    return jnp.concatenate(re, axis=0), jnp.concatenate(im, axis=0)


def polar_row(less_re, less_im, great_re, great_im, there, back):
    re = im = before = None
    for j in range(great_re.shape[0] // NW):
        rows = slice(j * NW, (j + 1) * NW)
        great = spectrum(there, great_re[rows], great_im[rows], 1)
        w_re, w_im = great if before is None else shifted(great, before)
        l_re, l_im = spectrum(there, less_re[rows], less_im[rows], -1)
        p_re = l_re * w_re - l_im * w_im
        p_im = l_re * w_im + l_im * w_re
        re, im = (p_re, p_im) if re is None else (re + p_re, im + p_im)
        before = great
    half = NW
    real = jnp.concatenate([re[:half] + re[half:], im[half:] - im[:half]], axis=0)
    imag = jnp.concatenate([im[:half] + im[half:], re[:half] - re[half:]], axis=0)
    high, low = split(jnp.concatenate([real, imag], axis=1))
    out = dot(back, jnp.concatenate([high, low, high], axis=0))
    return out[:, : re.shape[1]], out[:, re.shape[1] :]


def polar_kernel(less_hbm, great_hbm, there_hbm, back_hbm, out_ref, held, there, back, sems):
    rows = held.shape[1]

    def copy(which, i):
        source = (less_hbm, great_hbm)[which]
        return pltpu.make_async_copy(source.at[:, i], held.at[which, i], sems.at[which, i])

    fixed = (
        pltpu.make_async_copy(there_hbm, there, sems.at[0, rows]),
        pltpu.make_async_copy(back_hbm, back, sems.at[1, rows]),
    )
    for table in fixed:
        table.start()
    for i in range(rows):
        copy(0, i).start()
        copy(1, i).start()
    for table in fixed:
        table.wait()

    def row(i, carry):
        copy(0, i).wait()
        copy(1, i).wait()
        parts = [held[k, i, :, c].reshape(-1, held.shape[-1]) for k in range(2) for c in range(2)]
        for c, part in enumerate(polar_row(*parts, there[...], back[...])):
            wide = part.shape[1] // LANES
            for h in range(wide):
                place = pl.ds((c * wide + h) * rows + i, NW, stride=2 * wide * rows)
                out_ref[place, :] = part[:, h * LANES : (h + 1) * LANES]
        return carry

    lax.fori_loop(0, rows, row, 0)


def polar_of(less, great):
    sources, rows, _, local, columns = great.shape
    there, back = (jnp.asarray(t) for t in tables(NW))
    hbm = pl.BlockSpec(memory_space=pltpu.HBM)
    vmem = pl.BlockSpec(memory_space=pltpu.VMEM)
    out = pl.pallas_call(
        polar_kernel,
        in_specs=[hbm] * 4,
        out_specs=vmem,
        out_shape=jax.ShapeDtypeStruct((NW * 2 * rows * columns // LANES, LANES), jnp.float32),
        scratch_shapes=[
            pltpu.VMEM((2, rows, sources, 2, local, columns), jnp.float32),
            pltpu.VMEM(there.shape, there.dtype),
            pltpu.VMEM(back.shape, back.dtype),
            pltpu.SemaphoreType.DMA((2, rows + 1)),
        ],
        compiler_params=pltpu.CompilerParams(vmem_limit_bytes=57 * 1024 * 1024),
        cost_estimate=pl.CostEstimate(
            flops=4_000_000_000, bytes_accessed=9_500_000, transcendentals=0
        ),
    )(less, great, there, back)
    return out.reshape(NW, 2, columns // LANES, rows, LANES)


def tripled(x, axis, order):
    parts = split(x)
    return jnp.concatenate([parts[i] for i in order], axis=axis)


def sandwich(left, middle, right):
    left = tripled(left, 1, (0, 0, 1))
    right = tripled(right, 0, (0, 1, 0))
    halfway = [dot(left, tripled(m, 0, (0, 1, 0))) for m in middle]
    return [dot(tripled(h, 1, (0, 0, 1)), right) for h in halfway]


def block_of(ref, *index):
    wide = ref.shape[-3]
    return jnp.concatenate([ref[(slice(None), *index, h)].reshape(-1, LANES) for h in range(wide)], axis=1)


def screen(near, far, outer, v, w, w_t, a, a_t):
    terms = (sandwich(v, near, v), sandwich(w, far, w_t), sandwich(a, outer, a_t))
    return [x + y + z for x, y, z in zip(*terms)]


def pair_kernel(near, far, v, w, w_t, out_ref):
    blocks = [[block_of(ref, c) for c in range(2)] for ref in (near, far)]
    terms = sandwich(v[...], blocks[0], v[...]), sandwich(w[...], blocks[1], w_t[...])
    for c, (x, y) in enumerate(zip(*terms)):
        out_ref[c] = x + y


def send_kernel(c, part, outer, a, a_t, out_ref):
    (term,) = sandwich(a[...], [block_of(outer)], a_t[...])
    out_ref[...] = part[c] + term


def own_kernel(near, far, outer, v, w, w_t, a, a_t, out_ref):
    blocks = [[block_of(ref, c) for c in range(2)] for ref in (near, far, outer)]
    out_ref[0], out_ref[1] = screen(*blocks, v[...], w[...], w_t[...], a[...], a_t[...])


def on_core(body, shape, flops, *arrays):
    vmem = pl.BlockSpec(memory_space=pltpu.VMEM)
    return pl.pallas_call(
        body,
        in_specs=[vmem] * len(arrays),
        out_specs=vmem,
        out_shape=jax.ShapeDtypeStruct(shape, jnp.float32),
        compiler_params=pltpu.CompilerParams(vmem_limit_bytes=16 * 1024 * 1024),
        cost_estimate=pl.CostEstimate(
            flops=flops, bytes_accessed=sum(4 * x.size for x in arrays), transcendentals=0
        ),
    )(*arrays)


SWAP = [(0, 1), (1, 0)]


def plain(x):
    return with_layout_constraint(x, Layout(major_to_minor=tuple(range(x.ndim))))


def local(g_lesser, g_greater, v_diag, v_upper):
    devices = lax.axis_size(ENERGY)
    size = g_lesser.shape[3]
    rows = size // devices
    length = lax.axis_size("y")
    forward = [(i, i + 1) for i in range(length - 1)]

    first_core = lax.axis_index("core") == 0
    even = lax.axis_index("zl") == 0
    v, u = v_diag[0], v_upper[0]
    theirs = lax.ppermute(plain(jnp.where(first_core, v, u)), "zl", SWAP)
    less_send = g_lesser.reshape(2, -1, devices, rows, size).transpose(2, 0, 1, 3, 4)
    less = lax.all_to_all(lax.optimization_barrier(plain(less_send)), ENERGY, split_axis=0, concat_axis=0, tiled=True)
    less = plain(less)

    other = lax.ppermute(theirs, "core", SWAP)
    v_pair = jnp.where(first_core, theirs, other)
    u_pair = jnp.where(first_core, other, theirs)
    u0, u1 = jnp.where(even, u, u_pair), jnp.where(even, u_pair, u)
    before_t = plain(lax.ppermute(plain(u1), "y", forward)).T
    u0_t = u0.T
    w, w_t = jnp.where(even, u0_t, u0), jnp.where(even, u0, u0_t)
    sends, keeps = jnp.where(even, u1, before_t), jnp.where(even, before_t, u1)
    fixed = tuple(plain(x) for x in (v, v_pair, w, w_t, sends, sends.T, keeps, keeps.T))

    great_send = g_greater[:, :, 0].transpose(3, 0, 1, 2)
    great_send, fixed = lax.optimization_barrier((great_send, fixed))
    v_own, v_pair, w, w_t, sends, sends_t, keeps, keeps_t = fixed
    great = lax.all_to_all(great_send, ENERGY, split_axis=0, concat_axis=0, tiled=True)
    great = great.reshape((devices, rows) + great.shape[1:])

    polar = polar_of(plain(less.transpose(0, 3, 1, 2, 4)), great)
    polar = lax.all_to_all(
        plain(polar), ENERGY + ("zl",), split_axis=0, concat_axis=0, tiled=True
    )
    polar = polar.reshape((devices, PAIR) + polar.shape[1:])

    pair = [(i, l) for i in range(length) for l in range(PAIR)]
    number = {p: n for n, p in enumerate(pair)}
    toward, away = [], []
    for i, l in pair:
        step = 1 - 2 * l
        for route, target in ((toward, (i - step, l)), (away, (i + step, l))):
            if target in number:
                route.append((number[i, l], number[target]))
    near = plain(jnp.where(even, polar[:, 1], polar[:, 0]))
    far = plain(jnp.where(even, polar[:, 0], polar[:, 1]))
    for_send = []
    for c in range(2):
        for_send.append(lax.ppermute(plain(far[:, c]), SPACE, toward))
    for_own = lax.ppermute(near, SPACE, away)

    part = on_core(pair_kernel, (2, size, size), 800_000_000, near, far, v_pair, w, w_t)
    got = []
    for c in range(2):
        ready = on_core(
            functools.partial(send_kernel, c), (size, size), 200_000_000,
            part, for_send[c], sends, sends_t,
        )
        got.append(plain(lax.ppermute(plain(ready), "zl", SWAP)))
    kept = on_core(
        own_kernel, (2, size, size), 1_200_000_000, far, near, for_own, v_own, w_t, w, keeps, keeps_t
    )
    out = []
    for c in range(2):
        out += [jnp.where(even, kept[c], got[c]), jnp.where(even, got[c], kept[c])]
    return plain(jnp.stack(out).reshape(2, PAIR, 1, size, size))


def solution(mesh):
    count, width = mesh.devices.shape
    fine = Mesh(
        mesh.devices.reshape(count // CORES, CORES, width // PAIR, PAIR), ENERGY + SPACE
    )
    blocks = P(None, ENERGY, SPACE, None, None)
    rows = P(SPACE, None, None)
    return jax.shard_map(
        local, mesh=fine, in_specs=(blocks, blocks, rows, rows), out_specs=blocks, check_vma=False
    )
```
